32 devices in a mesh: data: 1 (over z), ctx: 32 (over y, x, core).
Axes of the slice: x: 4, y: 4, z: 1, core: 2. Of those that a mesh axis runs over, the one named last changes fastest.
The devices are a block of a 4x4x8 slice.
Arguments:
- hidden: bfloat16 [2048, 3584], P(('data', 'ctx'))
- seq_lens: int32 [2048], P(('data', 'ctx'))
- w_query: bfloat16 [2, 3584, 3584], replicated
- w_key: bfloat16 [2, 3584, 512], replicated
- w_value: bfloat16 [2, 3584, 512], replicated
- w_out: bfloat16 [2, 3584, 3584], replicated
- k_prefix: bfloat16 [2, 8192, 4, 128], P(None, ('data', 'ctx'))
- v_prefix: bfloat16 [2, 8192, 4, 128], P(None, ('data', 'ctx'))
- k_suffix: bfloat16 [2, 2048, 64, 4, 128], P(None, ('data', 'ctx'))
- v_suffix: bfloat16 [2, 2048, 64, 4, 128], P(None, ('data', 'ctx'))
Outputs:
- output 1: bfloat16 [2048, 3584], P(('data', 'ctx'))
- output 2: bfloat16 [2, 2048, 64, 4, 128], P(None, ('data', 'ctx'))
- output 3: bfloat16 [2, 2048, 64, 4, 128], P(None, ('data', 'ctx'))
All inputs are finite; a program needn't handle non-finite values.
Results may differ from the reference program's by a relative error of at most 0.00939984.
Values are sent between devices in bfloat16 or wider.
A program may use at most 768 MiB of HBM per device.

```python
import jax
import jax.numpy as jnp
from jax import lax

MODEL_DIM = 3584
NUM_HEADS = 28
KV_HEADS = 4
HEAD_DIM = 128
LAYERS = 2
SHARDS = 32
BATCH_SIZE = 2048
PREFIX_LEN = 8192
SUFFIX_LEN = 64
HOME_ROWS = 64


def setup_inputs(seed: int = 0, part: int = 0) -> dict:
    shared_keys = jax.random.split(jax.random.key(seed), 4)
    part_keys = jax.random.split(jax.random.fold_in(jax.random.key(seed + 1), part), 10)
    q_width = NUM_HEADS * HEAD_DIM
    kv_width = KV_HEADS * HEAD_DIM
    shard_rows = PREFIX_LEN // SHARDS
    w_query = jax.random.normal(shared_keys[0], (LAYERS, MODEL_DIM, q_width), jnp.float32) * MODEL_DIM ** -0.5
    w_key = jax.random.normal(shared_keys[1], (LAYERS, MODEL_DIM, kv_width), jnp.float32) * (2.5 * MODEL_DIM ** -0.5)
    w_value = jax.random.normal(shared_keys[2], (LAYERS, MODEL_DIM, kv_width), jnp.float32) * MODEL_DIM ** -0.5
    w_out = jax.random.normal(shared_keys[3], (LAYERS, q_width, MODEL_DIM), jnp.float32) * (q_width * LAYERS) ** -0.5
    hidden = jax.random.normal(part_keys[0], (BATCH_SIZE, MODEL_DIM), jnp.float32)
    centre_shape = (LAYERS, SHARDS, 1, KV_HEADS, HEAD_DIM)
    block_shape = (LAYERS, SHARDS, shard_rows, KV_HEADS, HEAD_DIM)
    prefix_shape = (LAYERS, PREFIX_LEN, KV_HEADS, HEAD_DIM)
    k_prefix = (1.5 * jax.random.normal(part_keys[1], centre_shape, jnp.float32) + jax.random.normal(part_keys[2], block_shape, jnp.float32)).reshape(prefix_shape)
    v_prefix = (jax.random.normal(part_keys[3], centre_shape, jnp.float32) + 0.5 * jax.random.normal(part_keys[4], block_shape, jnp.float32)).reshape(prefix_shape)
    seq_centre = (LAYERS, BATCH_SIZE, 1, KV_HEADS, HEAD_DIM)
    suffix_shape = (LAYERS, BATCH_SIZE, SUFFIX_LEN, KV_HEADS, HEAD_DIM)
    k_suffix = 2.5 * jax.random.normal(part_keys[5], seq_centre, jnp.float32) + jax.random.normal(part_keys[6], suffix_shape, jnp.float32)
    v_suffix = jax.random.normal(part_keys[7], seq_centre, jnp.float32) + 0.5 * jax.random.normal(part_keys[8], suffix_shape, jnp.float32)
    len_keys = jax.random.split(part_keys[9], 2)
    seq_lens = jax.random.randint(len_keys[0], (BATCH_SIZE,), 0, SUFFIX_LEN, dtype=jnp.int32)
    longest = jax.random.randint(len_keys[1], (), 0, BATCH_SIZE, dtype=jnp.int32)
    seq_lens = seq_lens.at[longest].set(SUFFIX_LEN - 1)
    seq_lens = seq_lens.at[(longest + BATCH_SIZE // 2) % BATCH_SIZE].set(0)
    return {'hidden': hidden.astype(jnp.bfloat16), 'seq_lens': seq_lens, 'w_query': w_query.astype(jnp.bfloat16), 'w_key': w_key.astype(jnp.bfloat16), 'w_value': w_value.astype(jnp.bfloat16), 'w_out': w_out.astype(jnp.bfloat16), 'k_prefix': k_prefix.astype(jnp.bfloat16), 'v_prefix': v_prefix.astype(jnp.bfloat16), 'k_suffix': k_suffix.astype(jnp.bfloat16), 'v_suffix': v_suffix.astype(jnp.bfloat16)}


def attend_block(queries, k_pre, v_pre, k_suf, v_suf, slot_live):
    score_scale = HEAD_DIM ** -0.5
    pre_scores = jnp.einsum('bkgd,pkd->bkgp', queries, k_pre) * score_scale
    suf_scores = jnp.einsum('bkgd,bskd->bkgs', queries, k_suf) * score_scale
    suf_scores = jnp.where(slot_live[:, None, None, :], suf_scores, -jnp.inf)
    row_max = jnp.maximum(pre_scores.max(axis=-1), suf_scores.max(axis=-1))
    pre_exp = jnp.exp(pre_scores - row_max[..., None])
    suf_exp = jnp.exp(suf_scores - row_max[..., None])
    mass_sum = pre_exp.sum(axis=-1) + suf_exp.sum(axis=-1)
    mixed_sum = jnp.einsum('bkgp,pkd->bkgd', pre_exp, v_pre) + jnp.einsum('bkgs,bskd->bkgd', suf_exp, v_suf)
    return mixed_sum / mass_sum[..., None]


def reference(hidden, seq_lens, w_query, w_key, w_value, w_out, k_prefix, v_prefix, k_suffix, v_suffix):
    group_size = NUM_HEADS // KV_HEADS
    blocks = BATCH_SIZE // HOME_ROWS
    slot_ids = jnp.arange(SUFFIX_LEN, dtype=jnp.int32)[None, :]
    slot_hit = (slot_ids == seq_lens[:, None])[:, :, None, None]
    slot_live = slot_ids <= seq_lens[:, None]
    live_blocks = slot_live.reshape(blocks, HOME_ROWS, SUFFIX_LEN)

    def layer_step(hidden_state, layer_args):
        q_weight, k_weight, v_weight, o_weight, k_pre, v_pre, k_suf, v_suf = layer_args
        queries = jnp.dot(hidden_state, q_weight, preferred_element_type=jnp.float32).astype(jnp.bfloat16)
        k_new = jnp.dot(hidden_state, k_weight, preferred_element_type=jnp.float32).astype(jnp.bfloat16).reshape(BATCH_SIZE, 1, KV_HEADS, HEAD_DIM)
        v_new = jnp.dot(hidden_state, v_weight, preferred_element_type=jnp.float32).astype(jnp.bfloat16).reshape(BATCH_SIZE, 1, KV_HEADS, HEAD_DIM)
        k_suf = jnp.where(slot_hit, k_new, k_suf)
        v_suf = jnp.where(slot_hit, v_new, v_suf)
        q_blocks = queries.astype(jnp.float32).reshape(blocks, HOME_ROWS, KV_HEADS, group_size, HEAD_DIM)
        k_full = k_pre.astype(jnp.float32)
        v_full = v_pre.astype(jnp.float32)
        k_blocks = k_suf.astype(jnp.float32).reshape(blocks, HOME_ROWS, SUFFIX_LEN, KV_HEADS, HEAD_DIM)
        v_blocks = v_suf.astype(jnp.float32).reshape(blocks, HOME_ROWS, SUFFIX_LEN, KV_HEADS, HEAD_DIM)
        attended = lax.map(lambda block_args: attend_block(block_args[0], k_full, v_full, block_args[1], block_args[2], block_args[3]), (q_blocks, k_blocks, v_blocks, live_blocks))
        attended = attended.astype(jnp.bfloat16).reshape(BATCH_SIZE, NUM_HEADS * HEAD_DIM)
        update = jnp.dot(attended, o_weight, preferred_element_type=jnp.float32).astype(jnp.bfloat16)
        hidden_state = (hidden_state.astype(jnp.float32) + update.astype(jnp.float32)).astype(jnp.bfloat16)
        return hidden_state, (k_suf, v_suf)

    hidden_out, cache_out = lax.scan(layer_step, hidden, (w_query, w_key, w_value, w_out, k_prefix, v_prefix, k_suffix, v_suffix))
    return hidden_out, cache_out[0], cache_out[1]
```

```python
import math

import jax
import jax.numpy as jnp
from jax import lax
from jax.experimental import pallas as pl
from jax.experimental.pallas import tpu as pltpu
from jax.sharding import PartitionSpec as P

CORES = 2
F32 = jnp.float32
BF16 = jnp.bfloat16
RING = 3
TILE_N = 512
SEQ_GROUP = 8
NT = (((1,), (1,)), ((), ()))


def build_kernel(layers, kvh, grp, hd, rows, model, shard, slots, side, ring):
    heads = kvh * grp
    qw = heads * hd
    kvw = kvh * hd
    qtiles = qw // TILE_N
    otiles = model // TILE_N
    pad_heads = -(-heads // 8) * 8
    hrows = grp * rows
    group_keys = side * shard
    half = shard // 2
    chunks = layers * kvh
    srows = slots * kvh
    ngroups = rows // SEQ_GROUP
    scale2 = hd ** -0.5 * math.log2(math.e)
    heads_per_tile = TILE_N // hd

    def kernel(lens_ref, x_in, wq, wk, wv, wo, kp, vp, ks, vs,
               x_out, kn_out, vn_out,
               kg, vg, wbuf, sbuf, xs, qh, qs, kn, vn, osuf, msuf, lsuf,
               s_ref, p_ref, m_ref, l_ref, acc_ref, attn, cslot, kslot,
               wsem, ssem_k, ssem_v, lsem, send_sem, recv_sem):
        me = lax.axis_index('ctx')
        core = me % CORES
        chip = me // CORES
        mx = chip % side
        my = chip // side

        def dev(y, x, c):
            return {'ctx': (y * side + x) * CORES + c}

        xp, xm = (mx + 1) % side, (mx + side - 1) % side
        yp, ym = (my + 1) % side, (my + side - 1) % side
        along_x = (dev(my, xp, core), dev(my, xm, core))
        along_y = (dev(yp, mx, core), dev(ym, mx, core))
        partner = dev(my, mx, 1 - core)

        kinds = ((kg, along_x, along_y, mx, my, xp, xm, yp, ym),
                 (vg, along_y, along_x, my, mx, yp, ym, xp, xm))

        def rdma(code, kind, chunk, src, dst, to):
            return pltpu.make_async_remote_copy(
                src_ref=src, dst_ref=dst,
                send_sem=send_sem.at[code, kind, chunk],
                recv_sem=recv_sem.at[code, kind, chunk],
                device_id=to, device_id_type=pl.DeviceIdType.MESH)

        def copies(step, kind, chunk, which):
            buf, d1, d2, a, b, ap, am, bp, bm = kinds[kind]
            l, h = chunk // kvh, chunk % kvh
            g = buf.at[l, h, core]
            lo, hi = pl.ds(0, half), pl.ds(half, half)
            q2 = side // 2
            glo, ghi = pl.ds(0, q2), pl.ds(q2, q2)
            a2 = (a + 2) % side
            b2 = (b + 2) % side
            out = []

            def add(code, src, to, dst_in):
                ref = src if which else dst_in
                out.append(rdma(code, kind, chunk, ref, ref, to))
            if step == 'x1':
                add(0, g.at[b, a], d1[0], g.at[b, am])
                add(1, g.at[b, a], d1[1], g.at[b, ap])
            elif step == 'x2':
                add(2, g.at[b, am, lo], d1[0], g.at[b, a2, lo])
                add(3, g.at[b, ap, hi], d1[1], g.at[b, a2, hi])
            elif step == 'y1':
                add(4, g.at[b], d2[0], g.at[bm])
                add(5, g.at[b], d2[1], g.at[bp])
            elif step == 'y2':
                add(6, g.at[bm, glo], d2[0], g.at[b2, glo])
                add(7, g.at[bp, ghi], d2[1], g.at[b2, ghi])
            else:
                other = buf.at[l, h, 1 - core]
                add(8, g, partner, other)
            return out

        def own_copy(kind, chunk):
            buf, d1, d2, a, b = kinds[kind][:5]
            l, h = chunk // kvh, chunk % kvh
            src = (kp, vp)[kind]
            return pltpu.make_async_copy(src.at[l, h], buf.at[l, h, core, b, a], lsem.at[kind, chunk])

        def send(step, chunk):
            for kind in range(2):
                for cp in copies(step, kind, chunk, 1):
                    cp.start()

        def recv(step, chunk):
            for kind in range(2):
                for cp in copies(step, kind, chunk, 0):
                    cp.wait_recv()

        def x1(i):
            for kind in range(2):
                own_copy(kind, i).wait()
            send('x1', i)

        def x2(i):
            recv('x1', i)
            send('x2', i)

        def y1(i):
            recv('x2', i)
            send('y1', i)

        def y2(i):
            recv('y1', i)
            send('y2', i)

        def dd(i):
            recv('y2', i)
            send('d', i)

        def ready(i):
            recv('d', i)

        per_layer = qtiles + 2 + otiles

        def wcopy(ref, l, n, slot):
            return pltpu.make_async_copy(ref.at[l, :, pl.ds(pl.multiple_of(n * TILE_N, TILE_N), TILE_N)],
                                         wbuf.at[slot], wsem.at[slot])

        def wstart(t):
            l, n, slot = t // per_layer, t % per_layer, t % ring

            @pl.when(n < qtiles)
            def _():
                wcopy(wq, l, n, slot).start()

            @pl.when(n == qtiles)
            def _():
                wcopy(wk, l, 0, slot).start()

            @pl.when(n == qtiles + 1)
            def _():
                wcopy(wv, l, 0, slot).start()

            @pl.when(n > qtiles + 1)
            def _():
                wcopy(wo, l, n - qtiles - 2, slot).start()

        def wtile(t, lhs_ref):
            slot = t % ring
            wcopy(wq, 0, 0, slot).wait()
            r = jnp.dot(lhs_ref[...], wbuf[slot], preferred_element_type=F32).astype(BF16)

            @pl.when(t + ring < layers * per_layer)
            def _():
                wstart(t + ring)
            return r

        def scopy(l, j, slot):
            n = SEQ_GROUP * srows
            rs = pl.ds(pl.multiple_of(j * n, n), n)
            return (pltpu.make_async_copy(ks.at[l, rs], sbuf.at[slot, 0], ssem_k.at[slot]),
                    pltpu.make_async_copy(vs.at[l, rs], sbuf.at[slot, 1], ssem_v.at[slot]))

        def own_start(i, carry):
            for kind in range(2):
                own_copy(kind, i).start()
            return carry
        lax.fori_loop(0, chunks, own_start, 0)

        def first_weights(t, carry):
            wstart(t)
            return carry
        lax.fori_loop(0, ring, first_weights, 0)
        barrier = pltpu.get_barrier_semaphore()
        for to in along_x + along_y + (partner,):
            pl.semaphore_signal(barrier, inc=1, device_id=to, device_id_type=pl.DeviceIdType.MESH)
        pl.semaphore_wait(barrier, 5)

        def x1_loop(i, carry):
            x1(i)
            return carry
        lax.fori_loop(0, kvh, x1_loop, 0)
        qs[...] = jnp.zeros_like(qs)
        xs[...] = x_in[...]

        row_head = lax.broadcasted_iota(jnp.int32, (pad_heads, srows), 0) // grp
        row_head = jnp.minimum(row_head, kvh - 1)
        col = lax.broadcasted_iota(jnp.int32, (pad_heads, srows), 1)
        col_slot_v = jnp.where(row_head == col % kvh, col // kvh, slots)
        cslot[...] = col_slot_v
        kslot[...] = lax.broadcasted_iota(jnp.int32, (srows, hd), 0) // kvh
        dup = 8 // kvh

        def suffix_group(j, slot):
            def one(b, carry):
                sb = j * SEQ_GROUP + b
                ln = lens_ref[sb]
                rws = pl.ds(pl.multiple_of(b * srows, srows), srows)
                hit = kslot[...] == ln

                def fresh(kv, new):
                    old = sbuf[slot, kv, rws, :].astype(F32)
                    nw = jnp.broadcast_to(new[sb][None], (srows // 8, 8, hd)).reshape(srows, hd)
                    return jnp.where(hit, nw, old).astype(BF16)
                kt = fresh(0, kn)
                vt = fresh(1, vn)
                s = lax.dot_general(qs[sb].astype(BF16), kt, NT, preferred_element_type=F32)
                s = jnp.where(cslot[...] <= ln, s, -jnp.inf)
                mm = jnp.max(s, axis=-1, keepdims=True)
                p = jnp.exp2(s * scale2 - mm * scale2)
                ll = jnp.sum(p, axis=-1, keepdims=True)
                osuf[sb] = jnp.dot(p.astype(BF16), vt, preferred_element_type=F32)
                msuf[sb] = jnp.broadcast_to(mm, (pad_heads, hd))
                lsuf[sb] = jnp.broadcast_to(ll * (1.0 / hd), (pad_heads, hd))
                return carry
            lax.fori_loop(0, SEQ_GROUP, one, 0, unroll=4)

        def grp_rows(g):
            return pl.ds(pl.multiple_of(g * rows, rows), rows)

        def attn_init(h):
            def one(g, carry):
                rs = grp_rows(g)
                hh = h * grp + g
                m_ref[rs, :] = msuf[:, hh, :]
                l_ref[rs, :] = lsuf[:, hh, :]
                acc_ref[rs, :] = osuf[:, hh, :]
                return carry
            lax.fori_loop(0, grp, one, 0)

        def where_is(idx):
            return (idx // side + core) % CORES, idx % side

        def scores(l, h, idx, buf):
            c, y = where_is(idx)
            for x in range(side):
                s_ref[buf, :, x * shard:(x + 1) * shard] = lax.dot_general(
                    qh[h], kg[l, h, c, y, x], NT, preferred_element_type=F32)

        def update(l, h, idx, buf):
            c, y = where_is(idx)

            def one(g, carry):
                rs = grp_rows(g)
                parts = [s_ref[buf, rs, j * 128:(j + 1) * 128] for j in range(group_keys // 128)]
                top = parts
                while len(top) > 1:
                    top = [jnp.maximum(a, b) for a, b in zip(top[::2], top[1::2])]
                m_old = m_ref[rs, :]
                m_new = jnp.maximum(m_old, jnp.max(top[0], axis=-1, keepdims=True))
                alpha = jnp.exp2((m_old - m_new) * scale2)
                mc = m_new * scale2
                tot = None
                for j, prt in enumerate(parts):
                    e = jnp.exp2(prt * scale2 - mc)
                    tot = e if tot is None else tot + e
                    p_ref[buf, rs, j * 128:(j + 1) * 128] = e.astype(BF16)
                m_ref[rs, :] = m_new
                l_ref[rs, :] = l_ref[rs, :] * alpha + tot
                acc_ref[rs, :] = acc_ref[rs, :] * alpha
                return carry
            lax.fori_loop(0, grp, one, 0, unroll=True)
            pv = None
            for x in range(side):
                d = jnp.dot(p_ref[buf, :, x * shard:(x + 1) * shard], vg[l, h, c, x, y],
                            preferred_element_type=F32)
                pv = d if pv is None else pv + d
            acc_ref[...] += pv

        def attn_final(h):
            def one(g, carry):
                rs = grp_rows(g)
                tot = jnp.sum(l_ref[rs, :], axis=-1, keepdims=True)
                hh = h * grp + g
                attn[:, pl.ds(pl.multiple_of(hh * hd, hd), hd)] = (acc_ref[rs, :] / tot).astype(BF16)
                return carry
            lax.fori_loop(0, grp, one, 0)

        groups = CORES * side

        def layer(l, carry):
            base = l * per_layer

            def qkv(n, carry):
                r = wtile(base + n, xs)

                @pl.when(n < qtiles)
                def _():
                    for j in range(heads_per_tile):
                        hh = n * heads_per_tile + j
                        part = r[:, j * hd:(j + 1) * hd]
                        qh[hh // grp, grp_rows(hh % grp), :] = part
                        qs[:, hh, :] = part.astype(F32)

                def new_rows(new, new_out):
                    new_out[l] = r
                    for h in range(kvh):
                        part = r[:, h * hd:(h + 1) * hd].astype(F32)
                        for d in range(dup):
                            new[:, d * kvh + h, :] = part

                @pl.when(n == qtiles)
                def _():
                    new_rows(kn, kn_out)
                    for cp in scopy(l, 0, 0):
                        cp.start()

                @pl.when(n == qtiles + 1)
                def _():
                    new_rows(vn, vn_out)

                @pl.when((l == 0) & (n >= 2) & (n < 2 + kvh))
                def _():
                    x2(n - 2)

                @pl.when((l == 0) & (n >= 2 + kvh) & (n < 4 + kvh))
                def _():
                    y1(n - 2 - kvh)

                @pl.when((l == 0) & (n == qtiles + 1))
                def _():
                    lax.fori_loop(kvh, chunks, x1_loop, 0)

                @pl.when((l == 1) & (n == qtiles + 1))
                def _():
                    dd(5)
                    y2(6)
                return carry
            lax.fori_loop(0, qtiles + 2, qkv, 0)

            def suf(j, carry):
                @pl.when(j + 1 < ngroups)
                def _():
                    for cp in scopy(l, j + 1, (j + 1) % 2):
                        cp.start()
                for cp in scopy(l, j, j % 2):
                    cp.wait()
                suffix_group(j, j % 2)

                @pl.when((l == 0) & (j >= 3) & (j < 3 + kvh))
                def _():
                    x2(kvh + j - 3)

                @pl.when((l == 0) & (j == ngroups - 1))
                def _():
                    y2(0)
                    y1(2)
                return carry
            lax.fori_loop(0, ngroups, suf, 0)

            def head(h, carry):
                i = l * kvh + h

                @pl.when(l == 0)
                def _():
                    dd(i)
                    y2(i + 1)
                    y1(i + 3)

                @pl.when(i == 5)
                def _():
                    dd(6)
                    y2(7)
                attn_init(h)
                scores(l, h, 0, 0)

                def pair(k, carry):
                    @pl.when(k == 1)
                    def _():
                        ready(i)
                    scores(l, h, 2 * k + 1, 1)
                    update(l, h, 2 * k, 0)
                    scores(l, h, 2 * k + 2, 0)
                    update(l, h, 2 * k + 1, 1)
                    return carry
                lax.fori_loop(0, groups // 2 - 1, pair, 0)
                scores(l, h, groups - 1, 1)
                update(l, h, groups - 2, 0)
                update(l, h, groups - 1, 1)

                @pl.when(i == 6)
                def _():
                    dd(7)
                attn_final(h)
                return carry
            lax.fori_loop(0, kvh, head, 0)

            def out(n, carry):
                r = wtile(base + qtiles + 2 + n, attn)
                cs = pl.ds(pl.multiple_of(n * TILE_N, TILE_N), TILE_N)
                xs[:, cs] = (xs[:, cs].astype(F32) + r.astype(F32)).astype(BF16)

                @pl.when((l == 0) & (n == otiles - 1))
                def _():
                    dd(4)
                    y2(5)
                    y1(7)
                return carry
            lax.fori_loop(0, otiles, out, 0)
            return carry
        lax.fori_loop(0, layers, layer, 0)
        x_out[...] = xs[...]

        def drain(i, carry):
            for step in ('x1', 'x2', 'y1', 'y2', 'd'):
                for kind in range(2):
                    for cp in copies(step, kind, i, 1):
                        cp.wait_send()
            return carry
        lax.fori_loop(0, chunks, drain, 0)

    scratch = [
        pltpu.VMEM((layers, kvh, CORES, side, side, shard, hd), BF16),
        pltpu.VMEM((layers, kvh, CORES, side, side, shard, hd), BF16),
        pltpu.VMEM((ring, max(model, qw), TILE_N), BF16),
        pltpu.VMEM((2, 2, SEQ_GROUP * srows, hd), BF16),
        pltpu.VMEM((rows, model), BF16),
        pltpu.VMEM((kvh, hrows, hd), BF16),
        pltpu.VMEM((rows, pad_heads, hd), F32),
        pltpu.VMEM((rows, 8, hd), F32),
        pltpu.VMEM((rows, 8, hd), F32),
        pltpu.VMEM((rows, pad_heads, hd), F32),
        pltpu.VMEM((rows, pad_heads, hd), F32),
        pltpu.VMEM((rows, pad_heads, hd), F32),
        pltpu.VMEM((2, hrows, group_keys), F32),
        pltpu.VMEM((2, hrows, group_keys), BF16),
        pltpu.VMEM((hrows, hd), F32),
        pltpu.VMEM((hrows, hd), F32),
        pltpu.VMEM((hrows, hd), F32),
        pltpu.VMEM((rows, qw), BF16),
        pltpu.VMEM((pad_heads, srows), jnp.int32),
        pltpu.VMEM((srows, hd), jnp.int32),
        pltpu.SemaphoreType.DMA((ring,)),
        pltpu.SemaphoreType.DMA((2,)),
        pltpu.SemaphoreType.DMA((2,)),
        pltpu.SemaphoreType.DMA((2, chunks)),
        pltpu.SemaphoreType.DMA((9, 2, chunks)),
        pltpu.SemaphoreType.DMA((9, 2, chunks)),
    ]
    return kernel, scratch


def solution(mesh):
    ctx_size = mesh.shape['ctx']
    side = math.isqrt(ctx_size // CORES)
    home_axes = ('data', 'ctx')
    row_spec = P(home_axes, None)
    lens_spec = P(home_axes)
    whole_spec = P()
    prefix_spec = P(None, home_axes, None, None)
    cache_spec = P(None, home_axes, None, None, None)

    def local_step(hidden, seq_lens, w_query, w_key, w_value, w_out, k_prefix, v_prefix, k_suffix, v_suffix):
        layers, shard, kvh, hd = k_prefix.shape
        rows, model = hidden.shape
        slots = k_suffix.shape[2]
        grp = w_query.shape[2] // hd // kvh
        kernel, scratch = build_kernel(layers, kvh, grp, hd, rows, model, shard, slots, side, RING)
        kp = jnp.swapaxes(k_prefix, 1, 2)
        vp = jnp.swapaxes(v_prefix, 1, 2)
        ks = k_suffix.reshape(layers, rows * slots * kvh, hd)
        vs = v_suffix.reshape(layers, rows * slots * kvh, hd)
        vmem = pl.BlockSpec(memory_space=pltpu.VMEM)
        hbm = pl.BlockSpec(memory_space=pl.ANY)
        x_new, k_new, v_new = pl.pallas_call(
            kernel,
            out_shape=(jax.ShapeDtypeStruct((rows, model), BF16),
                       jax.ShapeDtypeStruct((layers, rows, kvh * hd), BF16),
                       jax.ShapeDtypeStruct((layers, rows, kvh * hd), BF16)),
            in_specs=[pl.BlockSpec(memory_space=pltpu.SMEM), vmem] + [hbm] * 8,
            out_specs=(vmem, vmem, vmem),
            scratch_shapes=scratch,
            compiler_params=pltpu.CompilerParams(
                collective_id=0, has_side_effects=True, vmem_limit_bytes=67043328),
        )(seq_lens, hidden, w_query, w_key, w_value, w_out, kp, vp, ks, vs)
        slot_ids = lax.broadcasted_iota(jnp.int32, (rows, slots), 1)
        hit = (slot_ids == seq_lens[:, None])[None, :, :, None, None]
        k_out = jnp.where(hit, k_new.reshape(layers, rows, 1, kvh, hd), k_suffix)
        v_out = jnp.where(hit, v_new.reshape(layers, rows, 1, kvh, hd), v_suffix)
        return x_new, k_out, v_out

    return jax.shard_map(
        local_step, mesh=mesh,
        in_specs=(row_spec, lens_spec, whole_spec, whole_spec, whole_spec, whole_spec,
                  prefix_spec, prefix_spec, cache_spec, cache_spec),
        out_specs=(row_spec, cache_spec, cache_spec), check_vma=False)
```

```python
import functools
import math

import jax
import jax.numpy as jnp
from jax import lax
from jax.experimental import pallas as pl
from jax.experimental.pallas import tpu as pltpu
from jax.sharding import PartitionSpec as P

CORES = 2
F32 = jnp.float32
BF16 = jnp.bfloat16
RING = 3
TILE_N = 512
SEQ_GROUP = 8
SUF_SLOTS = 3
STEP = 32
EPI_GROUP = 8
NT = (((1,), (1,)), ((), ()))


def build_kernel(layers, kvh, grp, hd, rows, model, shard, slots, side, ring):
    heads = kvh * grp
    qw = heads * hd
    kvw = kvh * hd
    qtiles = qw // TILE_N
    otiles = model // TILE_N
    pad_heads = -(-heads // 8) * 8
    hrows = grp * rows
    group_keys = side * shard
    half = shard // 2
    chunks = layers * kvh
    srows = slots * kvh
    ngroups = rows // SEQ_GROUP
    scale2 = hd ** -0.5 * math.log2(math.e)
    heads_per_tile = TILE_N // hd

    def kernel(lens_ref, x_in, wq, wk, wv, wo, kp, vp, ks, vs,
               x_out, kn_out, vn_out,
               kg, vg, wbuf, sbuf, qh, qs,
               s_ref, p_ref, m_ref, l_ref, acc_ref, al_ref, mx_ref, attn, cslot, kslot,
               wsem, ssem_k, ssem_v, lsem, send_sem, recv_sem):
        me = lax.axis_index('ctx')
        core = me % CORES
        chip = me // CORES
        mx = chip % side
        my = chip // side

        def dev(y, x, c):
            return {'ctx': (y * side + x) * CORES + c}

        xp, xm = (mx + 1) % side, (mx + side - 1) % side
        yp, ym = (my + 1) % side, (my + side - 1) % side
        along_x = (dev(my, xp, core), dev(my, xm, core))
        along_y = (dev(yp, mx, core), dev(ym, mx, core))
        partner = dev(my, mx, 1 - core)

        kinds = ((kg, along_x, along_y, mx, my, xp, xm, yp, ym),
                 (vg, along_y, along_x, my, mx, yp, ym, xp, xm))

        def rdma(code, kind, chunk, src, dst, to):
            return pltpu.make_async_remote_copy(
                src_ref=src, dst_ref=dst,
                send_sem=send_sem.at[code, kind, chunk],
                recv_sem=recv_sem.at[code, kind, chunk],
                device_id=to, device_id_type=pl.DeviceIdType.MESH)

        def copies(step, kind, chunk, which):
            buf, d1, d2, a, b, ap, am, bp, bm = kinds[kind]
            l, h = chunk // kvh, chunk % kvh
            g = buf.at[l, h, core]
            lo, hi = pl.ds(0, half), pl.ds(half, half)
            q2 = side // 2
            glo, ghi = pl.ds(0, q2), pl.ds(q2, q2)
            a2 = (a + 2) % side
            b2 = (b + 2) % side
            out = []

            def add(code, src, to, dst_in):
                ref = src if which else dst_in
                out.append(rdma(code, kind, chunk, ref, ref, to))
            if step == 'x1':
                add(0, g.at[b, a], d1[0], g.at[b, am])
                add(1, g.at[b, a], d1[1], g.at[b, ap])
            elif step == 'x2':
                add(2, g.at[b, am, lo], d1[0], g.at[b, a2, lo])
                add(3, g.at[b, ap, hi], d1[1], g.at[b, a2, hi])
            elif step == 'y1':
                add(4, g.at[b], d2[0], g.at[bm])
                add(5, g.at[b], d2[1], g.at[bp])
            elif step == 'y2':
                add(6, g.at[bm, glo], d2[0], g.at[b2, glo])
                add(7, g.at[bp, ghi], d2[1], g.at[b2, ghi])
            else:
                other = buf.at[l, h, 1 - core]
                add(8, g, partner, other)
            return out

        def own_copy(kind, chunk):
            buf, d1, d2, a, b = kinds[kind][:5]
            l, h = chunk // kvh, chunk % kvh
            src = (kp, vp)[kind]
            return pltpu.make_async_copy(src.at[l, h], buf.at[l, h, core, b, a], lsem.at[kind, chunk])

        def send(step, chunk):
            for kind in range(2):
                for cp in copies(step, kind, chunk, 1):
                    cp.start()

        def recv(step, chunk):
            for kind in range(2):
                for cp in copies(step, kind, chunk, 0):
                    cp.wait_recv()

        def x1(i):
            for kind in range(2):
                own_copy(kind, i).wait()
            send('x1', i)

        def x2(i):
            recv('x1', i)
            send('x2', i)

        def y1(i):
            recv('x2', i)
            send('y1', i)

        def y2(i):
            recv('y1', i)
            send('y2', i)

        def dd(i):
            recv('y2', i)
            send('d', i)

        def ready(i):
            recv('d', i)

        per_layer = qtiles + 2 + otiles

        def wcopy(ref, l, n, slot):
            return pltpu.make_async_copy(ref.at[l, :, pl.ds(pl.multiple_of(n * TILE_N, TILE_N), TILE_N)],
                                         wbuf.at[slot], wsem.at[slot])

        def wstart(t):
            l, n, slot = t // per_layer, t % per_layer, t % ring

            @pl.when(n < qtiles)
            def _():
                wcopy(wq, l, n, slot).start()

            @pl.when(n == qtiles)
            def _():
                wcopy(wk, l, 0, slot).start()

            @pl.when(n == qtiles + 1)
            def _():
                wcopy(wv, l, 0, slot).start()

            @pl.when(n > qtiles + 1)
            def _():
                wcopy(wo, l, n - qtiles - 2, slot).start()

        def wtile(t, lhs_ref):
            slot = t % ring
            wcopy(wq, 0, 0, slot).wait()
            r = jnp.dot(lhs_ref[...], wbuf[slot], preferred_element_type=F32).astype(BF16)

            @pl.when(t + ring < layers * per_layer)
            def _():
                wstart(t + ring)
            return r

        def scopy(t):
            l, j, slot = t // ngroups, t % ngroups, t % SUF_SLOTS
            n = SEQ_GROUP * srows
            rs = pl.ds(pl.multiple_of(j * n, n), n)
            return (pltpu.make_async_copy(ks.at[l, rs], sbuf.at[slot, 0], ssem_k.at[slot]),
                    pltpu.make_async_copy(vs.at[l, rs], sbuf.at[slot, 1], ssem_v.at[slot]))

        def own_start(i, carry):
            for kind in range(2):
                own_copy(kind, i).start()
            return carry
        lax.fori_loop(0, chunks, own_start, 0)

        def first_weights(t, carry):
            wstart(t)
            return carry
        lax.fori_loop(0, ring, first_weights, 0)

        def first_suffix(t, carry):
            for cp in scopy(t):
                cp.start()
            return carry
        lax.fori_loop(0, SUF_SLOTS, first_suffix, 0)
        barrier = pltpu.get_barrier_semaphore()
        for to in along_x + along_y + (partner,):
            pl.semaphore_signal(barrier, inc=1, device_id=to, device_id_type=pl.DeviceIdType.MESH)
        pl.semaphore_wait(barrier, 5)

        def x1_loop(i, carry):
            x1(i)
            return carry
        lax.fori_loop(0, 2, x1_loop, 0)
        qs[...] = jnp.zeros_like(qs)
        x_out[...] = x_in[...]

        row_head = lax.broadcasted_iota(jnp.int32, (pad_heads, srows), 0) // grp
        row_head = jnp.minimum(row_head, kvh - 1)
        col = lax.broadcasted_iota(jnp.int32, (pad_heads, srows), 1)
        col_slot_v = jnp.where(row_head == col % kvh, col // kvh, slots)
        cslot[...] = col_slot_v
        kslot[...] = lax.broadcasted_iota(jnp.int32, (srows, hd), 0) // kvh
        dup = 8 // kvh

        def suffix_group(l, j, slot):
            lns, krows, vrows, qrows, outs = [], [], [], [], []
            for b in range(SEQ_GROUP):
                sb = j * SEQ_GROUP + b
                ln = lens_ref[sb]
                hit = kslot[...] == ln
                rws = slice(b * srows, (b + 1) * srows)

                def fresh(kv, new):
                    old = sbuf[slot, kv, rws, :].astype(F32)
                    nw = jnp.broadcast_to(new[l, sb][None], (srows // 8, 8, hd)).reshape(srows, hd)
                    return jnp.where(hit, nw, old).astype(BF16)
                lns.append(ln)
                krows.append(fresh(0, kn_out))
                vrows.append(fresh(1, vn_out))
                qrows.append(pl.ds(pl.multiple_of(sb * pad_heads, pad_heads), pad_heads))
            sc = [lax.dot_general(qs[qrows[b], :].astype(BF16), krows[b], NT, preferred_element_type=F32)
                  for b in range(SEQ_GROUP)]
            for b in range(SEQ_GROUP):
                s = jnp.where(cslot[...] <= lns[b], sc[b], -jnp.inf)
                mm = jnp.max(s, axis=-1, keepdims=True)
                p = jnp.exp2(s * scale2 - mm * scale2)
                ll = jnp.sum(p, axis=-1, keepdims=True)
                outs.append((mm, ll, p.astype(BF16)))
            vals = [jnp.dot(outs[b][2], vrows[b], preferred_element_type=F32) for b in range(SEQ_GROUP)]
            first = pl.ds(pl.multiple_of(j * SEQ_GROUP, SEQ_GROUP), SEQ_GROUP)
            for dst, per_seq in ((acc_ref, vals),
                                 (m_ref, [jnp.broadcast_to(o[0], (pad_heads, hd)) for o in outs]),
                                 (l_ref, [jnp.broadcast_to(o[1] * (1.0 / hd), (pad_heads, hd)) for o in outs])):
                for t in range(0, pad_heads, 8):
                    block = jnp.swapaxes(jnp.stack([a[t:t + 8] for a in per_seq], axis=0), 0, 1)
                    for hh in range(t, min(t + 8, heads)):
                        dst[hh, first, :] = block[hh - t]

        def grp_rows(g):
            return pl.ds(pl.multiple_of(g * rows, rows), rows)

        def where_is(idx):
            return (idx // side + core) % CORES, idx % side

        def scores(l, h, idx, buf):
            c, y = where_is(idx)
            top = None
            for x in range(side):
                d = lax.dot_general(qh[h], kg[l, h, c, y, x], NT, preferred_element_type=F32)
                s_ref[buf, :, x * shard:(x + 1) * shard] = d
                for j in range(shard // 128):
                    part = d[:, j * 128:(j + 1) * 128]
                    top = part if top is None else jnp.maximum(top, part)
            mx_ref[buf] = top

        def soften(h, buf):
            def one(g, carry):
                rs = grp_rows(g)
                hh = h * grp + g
                m_old = m_ref[hh]
                m_new = jnp.maximum(m_old, jnp.max(mx_ref[buf, rs, :], axis=-1, keepdims=True))
                alpha = jnp.exp2((m_old - m_new) * scale2)
                mc = m_new * scale2
                tot = None
                for j in range(group_keys // 128):
                    e = jnp.exp2(s_ref[buf, rs, j * 128:(j + 1) * 128] * scale2 - mc)
                    tot = e if tot is None else tot + e
                    p_ref[buf, rs, j * 128:(j + 1) * 128] = e.astype(BF16)
                m_ref[hh] = m_new
                l_ref[hh] = l_ref[hh] * alpha + tot
                al_ref[buf, rs, :] = alpha
                return carry
            lax.fori_loop(0, grp, one, 0, unroll=True)

        def mix(l, h, idx, buf):
            c, y = where_is(idx)
            pv = None
            for x in range(side):
                d = jnp.dot(p_ref[buf, :, x * shard:(x + 1) * shard], vg[l, h, c, x, y],
                            preferred_element_type=F32)
                pv = d if pv is None else pv + d
            for g in range(grp):
                rs = slice(g * rows, (g + 1) * rows)
                acc_ref[h * grp + g] = acc_ref[h * grp + g] * al_ref[buf, rs, :] + pv[rs]

        def attn_final(h):
            def one(g, carry):
                tot = jnp.sum(l_ref[h * grp + g], axis=-1, keepdims=True)
                hh = h * grp + g
                attn[:, pl.ds(pl.multiple_of(hh * hd, hd), hd)] = (acc_ref[h * grp + g] / tot).astype(BF16)
                return carry
            lax.fori_loop(0, grp, one, 0, unroll=True)

        groups = CORES * side

        def layer(l, carry):
            base = l * per_layer

            def qkv(n, carry):
                r = wtile(base + n, x_out)

                @pl.when(n < qtiles)
                def _():
                    for j in range(heads_per_tile):
                        hh = n * heads_per_tile + j
                        part = r[:, j * hd:(j + 1) * hd]
                        qh[hh // grp, grp_rows(hh % grp), :] = part
                        qs[pl.ds(hh, rows, stride=pad_heads), :] = part.astype(F32)

                def new_rows(new):
                    for h in range(kvh):
                        part = r[:, h * hd:(h + 1) * hd].astype(F32)
                        for d in range(dup):
                            new[l, :, d * kvh + h, :] = part

                @pl.when(n == qtiles)
                def _():
                    new_rows(kn_out)

                @pl.when(n == qtiles + 1)
                def _():
                    new_rows(vn_out)

                @pl.when((l == 0) & (n >= 2) & (n < 2 + kvh))
                def _():
                    x2(n - 2)

                @pl.when((l == 0) & (n >= 2) & (n < kvh))
                def _():
                    x1(n)

                @pl.when((l == 0) & (n == kvh))
                def _():
                    y1(0)

                @pl.when((l == 0) & (n == qtiles + 1))
                def _():
                    y2(0)
                    y1(1)

                @pl.when((l == 1) & (n == 2))
                def _():
                    dd(4)

                @pl.when((l == 1) & (n == qtiles - 1))
                def _():
                    y1(7)

                @pl.when((l == 1) & (n == qtiles + 1))
                def _():
                    dd(5)
                    y2(6)

                return carry
            lax.fori_loop(0, qtiles + 2, qkv, 0)

            def suf(j, carry):
                t = l * ngroups + j
                for cp in scopy(t):
                    cp.wait()
                suffix_group(l, j, t % SUF_SLOTS)

                @pl.when(t + SUF_SLOTS < layers * ngroups)
                def _():
                    for cp in scopy(t + SUF_SLOTS):
                        cp.start()

                @pl.when((l == 0) & (j == ngroups - 1))
                def _():
                    y1(2)

                return carry
            lax.fori_loop(0, ngroups, suf, 0)

            def head(h, carry):
                i = l * kvh + h

                @pl.when(l == 0)
                def _():
                    dd(h)

                @pl.when(i == 6)
                def _():
                    dd(7)

                scores(l, h, 0, 0)
                scores(l, h, 1, 1)
                soften(h, 0)

                def pair(k, carry):
                    @pl.when(k == groups // 4 - 1)
                    def _():
                        ready(i)

                        @pl.when(i == 0)
                        def _():
                            y2(1)
                            y1(3)
                            x1(4)

                        @pl.when(i == 1)
                        def _():
                            y2(2)
                            x2(4)
                            x1(5)

                        @pl.when(i == 2)
                        def _():
                            y2(3)
                            y1(4)
                            x2(5)

                        @pl.when(i == 3)
                        def _():
                            y1(5)
                            x1(6)
                            x1(7)

                        @pl.when(i == 4)
                        def _():
                            dd(6)
                            y2(7)
                    scores(l, h, 2 * k + 2, 0)
                    soften(h, 1)
                    mix(l, h, 2 * k, 0)
                    scores(l, h, 2 * k + 3, 1)
                    soften(h, 0)
                    mix(l, h, 2 * k + 1, 1)
                    return carry
                lax.fori_loop(0, groups // 2 - 1, pair, 0)
                soften(h, 1)
                mix(l, h, groups - 2, 0)
                mix(l, h, groups - 1, 1)

                attn_final(h)

                @pl.when(i == kvh - 1)
                def _():
                    y2(4)
                    x2(6)
                    x2(7)

                return carry
            lax.fori_loop(0, kvh, head, 0)

            def out(n, carry):
                r = wtile(base + qtiles + 2 + n, attn)
                cs = pl.ds(pl.multiple_of(n * TILE_N, TILE_N), TILE_N)
                x_out[:, cs] = (x_out[:, cs].astype(F32) + r.astype(F32)).astype(BF16)

                @pl.when((l == 0) & (n == otiles - 1))
                def _():
                    y2(5)
                    y1(6)

                return carry
            lax.fori_loop(0, otiles, out, 0)
            return carry
        lax.fori_loop(0, layers, layer, 0)

        def drain(i, carry):
            for step in ('x1', 'x2', 'y1', 'y2', 'd'):
                for kind in range(2):
                    for cp in copies(step, kind, i, 1):
                        cp.wait_send()
            return carry
        lax.fori_loop(0, chunks, drain, 0)

    scratch = [
        pltpu.VMEM((layers, kvh, CORES, side, side, shard, hd), BF16),
        pltpu.VMEM((layers, kvh, CORES, side, side, shard, hd), BF16),
        pltpu.VMEM((ring, max(model, qw), TILE_N), BF16),
        pltpu.VMEM((SUF_SLOTS, 2, SEQ_GROUP * srows, hd), BF16),
        pltpu.VMEM((kvh, hrows, hd), BF16),
        pltpu.VMEM((rows * pad_heads, hd), F32),
        pltpu.VMEM((2, hrows, group_keys), F32),
        pltpu.VMEM((2, hrows, group_keys), BF16),
        pltpu.VMEM((heads, rows, hd), F32),
        pltpu.VMEM((heads, rows, hd), F32),
        pltpu.VMEM((heads, rows, hd), F32),
        pltpu.VMEM((2, hrows, hd), F32),
        pltpu.VMEM((2, hrows, hd), F32),
        pltpu.VMEM((rows, qw), BF16),
        pltpu.VMEM((pad_heads, srows), jnp.int32),
        pltpu.VMEM((srows, hd), jnp.int32),
        pltpu.SemaphoreType.DMA((ring,)),
        pltpu.SemaphoreType.DMA((SUF_SLOTS,)),
        pltpu.SemaphoreType.DMA((SUF_SLOTS,)),
        pltpu.SemaphoreType.DMA((2, chunks)),
        pltpu.SemaphoreType.DMA((9, 2, chunks)),
        pltpu.SemaphoreType.DMA((9, 2, chunks)),
    ]
    return kernel, scratch


def fresh_caches(lens_ref, k_ref, v_ref, kn_ref, vn_ref, k_out, v_out, kbuf, vbuf, kn_buf, vn_buf, in_sem, out_sem, new_sem, *, kvh):
    layers, rows = kn_ref.shape[:2]
    slots = k_ref.shape[1] // rows
    n = EPI_GROUP * slots
    steps = rows // EPI_GROUP

    def copies(t, out):
        l, j = t // steps, t % steps
        rs = pl.ds(j * n, n)
        sem = out_sem if out else in_sem
        res = []
        for i, (src, buf, dst) in enumerate(((k_ref, kbuf, k_out), (v_ref, vbuf, v_out))):
            if out:
                res.append(pltpu.make_async_copy(buf.at[t], dst.at[l, rs], sem.at[i, t]))
            else:
                res.append(pltpu.make_async_copy(src.at[l, rs], buf.at[t], sem.at[i, t]))
        return res

    def start(t, carry):
        for cp in copies(t, False):
            cp.start()
        return carry

    def patch(t, carry):
        for cp in copies(t, False):
            cp.wait()
        l, j = t // steps, t % steps
        for b in range(EPI_GROUP):
            sb = j * EPI_GROUP + b
            at = b * slots + lens_ref[sb]
            kbuf[t, at] = kn_buf[l, sb, :kvh, :].astype(BF16)
            vbuf[t, at] = vn_buf[l, sb, :kvh, :].astype(BF16)
        for cp in copies(t, True):
            cp.start()
        return carry

    def finish(t, carry):
        for cp in copies(t, True):
            cp.wait()
        return carry
    news = [pltpu.make_async_copy(kn_ref, kn_buf, new_sem.at[0]), pltpu.make_async_copy(vn_ref, vn_buf, new_sem.at[1])]
    for cp in news:
        cp.start()
    lax.fori_loop(0, layers * steps, start, 0)
    for cp in news:
        cp.wait()
    lax.fori_loop(0, layers * steps, patch, 0)
    lax.fori_loop(0, layers * steps, finish, 0)


def solution(mesh):
    ctx_size = mesh.shape['ctx']
    side = math.isqrt(ctx_size // CORES)
    home_axes = ('data', 'ctx')
    row_spec = P(home_axes, None)
    lens_spec = P(home_axes)
    whole_spec = P()
    prefix_spec = P(None, home_axes, None, None)
    cache_spec = P(None, home_axes, None, None, None)

    def local_step(hidden, seq_lens, w_query, w_key, w_value, w_out, k_prefix, v_prefix, k_suffix, v_suffix):
        layers, shard, kvh, hd = k_prefix.shape
        rows, model = hidden.shape
        slots = k_suffix.shape[2]
        grp = w_query.shape[2] // hd // kvh
        kernel, scratch = build_kernel(layers, kvh, grp, hd, rows, model, shard, slots, side, RING)
        kp = jnp.swapaxes(k_prefix, 1, 2)
        vp = jnp.swapaxes(v_prefix, 1, 2)
        ks = k_suffix.reshape(layers, rows * slots * kvh, hd)
        vs = v_suffix.reshape(layers, rows * slots * kvh, hd)
        vmem = pl.BlockSpec(memory_space=pltpu.VMEM)
        hbm = pl.BlockSpec(memory_space=pl.ANY)
        x_new, k_new, v_new = pl.pallas_call(
            kernel,
            out_shape=(jax.ShapeDtypeStruct((rows, model), BF16),
                       jax.ShapeDtypeStruct((layers, rows, 8, hd), F32),
                       jax.ShapeDtypeStruct((layers, rows, 8, hd), F32)),
            in_specs=[pl.BlockSpec(memory_space=pltpu.SMEM), vmem] + [hbm] * 8,
            out_specs=(vmem, vmem, vmem),
            scratch_shapes=scratch,
            compiler_params=pltpu.CompilerParams(
                collective_id=0, has_side_effects=True, vmem_limit_bytes=67043328),
        )(seq_lens, hidden, w_query, w_key, w_value, w_out, kp, vp, ks, vs)
        steps = layers * (rows // EPI_GROUP)
        flat = (layers, rows * slots, kvh, hd)
        k_out, v_out = pl.pallas_call(
            functools.partial(fresh_caches, kvh=kvh),
            out_shape=(jax.ShapeDtypeStruct(flat, BF16),) * 2,
            in_specs=[pl.BlockSpec(memory_space=pltpu.SMEM), hbm, hbm]
            + [pl.BlockSpec(memory_space=pltpu.HBM)] * 2,
            out_specs=(hbm, hbm),
            scratch_shapes=[pltpu.VMEM((steps, EPI_GROUP * slots, kvh, hd), BF16)] * 2
            + [pltpu.VMEM(k_new.shape, F32)] * 2 + [pltpu.SemaphoreType.DMA((2, steps))] * 2
            + [pltpu.SemaphoreType.DMA((2,))],
            compiler_params=pltpu.CompilerParams(vmem_limit_bytes=48 * 2 ** 20),
        )(seq_lens, k_suffix.reshape(flat), v_suffix.reshape(flat), k_new, v_new)
        k_out = k_out.reshape(k_suffix.shape)
        v_out = v_out.reshape(v_suffix.shape)
        return x_new, k_out, v_out

    return jax.shard_map(
        local_step, mesh=mesh,
        in_specs=(row_spec, lens_spec, whole_spec, whole_spec, whole_spec, whole_spec,
                  prefix_spec, prefix_spec, cache_spec, cache_spec),
        out_specs=(row_spec, cache_spec, cache_spec), check_vma=False)
```

```python
import functools
import math

import jax
import jax.numpy as jnp
from jax import lax
from jax.experimental import pallas as pl
from jax.experimental.pallas import tpu as pltpu
from jax.sharding import PartitionSpec as P

CORES = 2
F32 = jnp.float32
BF16 = jnp.bfloat16
RING = 3
TILE_N = 512
SEQ_GROUP = 8
SUF_SLOTS = 3
EPI_GROUP = 8
NT = (((1,), (1,)), ((), ()))


def build_kernel(layers, kvh, grp, hd, rows, model, shard, slots, side, ring):
    heads = kvh * grp
    qw = heads * hd
    kvw = kvh * hd
    qtiles = qw // TILE_N
    otiles = model // TILE_N
    pad_heads = -(-heads // 8) * 8
    hrows = grp * rows
    group_keys = side * shard
    half = shard // 2
    chunks = layers * kvh
    srows = slots * kvh
    ngroups = rows // SEQ_GROUP
    scale2 = hd ** -0.5 * math.log2(math.e)
    heads_per_tile = TILE_N // hd

    def kernel(lens_ref, x_in, wq, wk, wv, wo, kp, vp, ks, vs,
               x_out, kn_out, vn_out,
               kg, vg, wbuf, sbuf, qh, qs,
               s_ref, p_ref, m_ref, l_ref, acc_ref, al_ref, attn, cslot, kslot,
               wsem, ssem_k, ssem_v, lsem, send_sem, recv_sem):
        me = lax.axis_index('ctx')
        core = me % CORES
        chip = me // CORES
        mx = chip % side
        my = chip // side

        def dev(y, x, c):
            return {'ctx': (y * side + x) * CORES + c}

        xp, xm = (mx + 1) % side, (mx + side - 1) % side
        yp, ym = (my + 1) % side, (my + side - 1) % side
        along_x = (dev(my, xp, core), dev(my, xm, core))
        along_y = (dev(yp, mx, core), dev(ym, mx, core))
        partner = dev(my, mx, 1 - core)

        kinds = ((kg, along_x, along_y, mx, my, xp, xm, yp, ym),
                 (vg, along_y, along_x, my, mx, yp, ym, xp, xm))

        def rdma(code, kind, chunk, src, dst, to):
            return pltpu.make_async_remote_copy(
                src_ref=src, dst_ref=dst,
                send_sem=send_sem.at[code, kind, chunk],
                recv_sem=recv_sem.at[code, kind, chunk],
                device_id=to, device_id_type=pl.DeviceIdType.MESH)

        def copies(step, kind, chunk, which):
            buf, d1, d2, a, b, ap, am, bp, bm = kinds[kind]
            l, h = chunk // kvh, chunk % kvh
            g = buf.at[l, h, core]
            lo, hi = pl.ds(0, half), pl.ds(half, half)
            q2 = side // 2
            glo, ghi = pl.ds(0, q2), pl.ds(q2, q2)
            a2 = (a + 2) % side
            b2 = (b + 2) % side
            out = []

            def add(code, src, to, dst_in):
                ref = src if which else dst_in
                out.append(rdma(code, kind, chunk, ref, ref, to))
            if step == 'x1':
                add(0, g.at[b, a], d1[0], g.at[b, am])
                add(1, g.at[b, a], d1[1], g.at[b, ap])
            elif step == 'x2':
                add(2, g.at[b, am, lo], d1[0], g.at[b, a2, lo])
                add(3, g.at[b, ap, hi], d1[1], g.at[b, a2, hi])
            elif step == 'y1':
                add(4, g.at[b], d2[0], g.at[bm])
                add(5, g.at[b], d2[1], g.at[bp])
            elif step == 'y2':
                add(6, g.at[bm, glo], d2[0], g.at[b2, glo])
                add(7, g.at[bp, ghi], d2[1], g.at[b2, ghi])
            else:
                other = buf.at[l, h, 1 - core]
                add(8, g, partner, other)
            return out

        def own_copy(kind, chunk):
            buf, d1, d2, a, b = kinds[kind][:5]
            l, h = chunk // kvh, chunk % kvh
            src = (kp, vp)[kind]
            return pltpu.make_async_copy(src.at[l, h], buf.at[l, h, core, b, a], lsem.at[kind, chunk])

        def send(step, chunk):
            for kind in range(2):
                for cp in copies(step, kind, chunk, 1):
                    cp.start()

        def recv(step, chunk):
            for kind in range(2):
                for cp in copies(step, kind, chunk, 0):
                    cp.wait_recv()

        def x1(i):
            for kind in range(2):
                own_copy(kind, i).wait()
            send('x1', i)

        def x2(i):
            recv('x1', i)
            send('x2', i)

        def y1(i):
            recv('x2', i)
            send('y1', i)

        def y2(i):
            recv('y1', i)
            send('y2', i)

        def dd(i):
            recv('y2', i)
            send('d', i)

        def ready(i):
            recv('d', i)

        per_layer = qtiles + 2 + otiles

        def wcopy(ref, l, n, slot):
            return pltpu.make_async_copy(ref.at[l, :, pl.ds(pl.multiple_of(n * TILE_N, TILE_N), TILE_N)],
                                         wbuf.at[slot], wsem.at[slot])

        def wstart(t):
            l, n, slot = t // per_layer, t % per_layer, t % ring

            @pl.when(n < qtiles)
            def _():
                wcopy(wq, l, n, slot).start()

            @pl.when(n == qtiles)
            def _():
                wcopy(wk, l, 0, slot).start()

            @pl.when(n == qtiles + 1)
            def _():
                wcopy(wv, l, 0, slot).start()

            @pl.when(n > qtiles + 1)
            def _():
                wcopy(wo, l, n - qtiles - 2, slot).start()

        def wtile(t, lhs_ref):
            slot = t % ring
            wcopy(wq, 0, 0, slot).wait()
            r = jnp.dot(lhs_ref[...], wbuf[slot], preferred_element_type=F32).astype(BF16)

            @pl.when(t + ring < layers * per_layer)
            def _():
                wstart(t + ring)
            return r

        def scopy(t):
            l, j, slot = t // ngroups, t % ngroups, t % SUF_SLOTS
            n = SEQ_GROUP * srows
            rs = pl.ds(pl.multiple_of(j * n, n), n)
            return (pltpu.make_async_copy(ks.at[l, rs], sbuf.at[slot, 0], ssem_k.at[slot]),
                    pltpu.make_async_copy(vs.at[l, rs], sbuf.at[slot, 1], ssem_v.at[slot]))

        def own_start(i, carry):
            for kind in range(2):
                own_copy(kind, i).start()
            return carry
        lax.fori_loop(0, chunks, own_start, 0)

        def first_weights(t, carry):
            wstart(t)
            return carry
        lax.fori_loop(0, ring, first_weights, 0)

        def first_suffix(t, carry):
            for cp in scopy(t):
                cp.start()
            return carry
        lax.fori_loop(0, SUF_SLOTS, first_suffix, 0)
        barrier = pltpu.get_barrier_semaphore()
        for to in along_x + along_y + (partner,):
            pl.semaphore_signal(barrier, inc=1, device_id=to, device_id_type=pl.DeviceIdType.MESH)
        pl.semaphore_wait(barrier, 5)

        def x1_loop(i, carry):
            x1(i)
            return carry
        lax.fori_loop(0, 2, x1_loop, 0)
        qs[...] = jnp.zeros_like(qs)
        x_out[...] = x_in[...]

        row_head = lax.broadcasted_iota(jnp.int32, (pad_heads, srows), 0) // grp
        row_head = jnp.minimum(row_head, kvh - 1)
        col = lax.broadcasted_iota(jnp.int32, (pad_heads, srows), 1)
        col_slot_v = jnp.where(row_head == col % kvh, col // kvh, slots)
        cslot[...] = col_slot_v
        kslot[...] = lax.broadcasted_iota(jnp.int32, (srows, hd), 0) // kvh
        dup = 8 // kvh

        def suffix_group(l, j, slot):
            lns, krows, vrows, qrows, outs = [], [], [], [], []
            for b in range(SEQ_GROUP):
                sb = j * SEQ_GROUP + b
                ln = lens_ref[sb]
                hit = kslot[...] == ln
                rws = slice(b * srows, (b + 1) * srows)

                def fresh(kv, new):
                    old = sbuf[slot, kv, rws, :].astype(F32)
                    nw = jnp.broadcast_to(new[l, sb][None], (srows // 8, 8, hd)).reshape(srows, hd)
                    return jnp.where(hit, nw, old).astype(BF16)
                lns.append(ln)
                krows.append(fresh(0, kn_out))
                vrows.append(fresh(1, vn_out))
                qrows.append(pl.ds(pl.multiple_of(sb * pad_heads, pad_heads), pad_heads))
            sc = [lax.dot_general(qs[qrows[b], :].astype(BF16), krows[b], NT, preferred_element_type=F32)
                  for b in range(SEQ_GROUP)]
            for b in range(SEQ_GROUP):
                s = jnp.where(cslot[...] <= lns[b], sc[b], -jnp.inf)
                mm = jnp.max(s, axis=-1, keepdims=True)
                p = jnp.exp2(s * scale2 - mm * scale2)
                ll = jnp.sum(p, axis=-1, keepdims=True)
                outs.append((mm, ll, p.astype(BF16)))
            vals = [jnp.dot(outs[b][2], vrows[b], preferred_element_type=F32) for b in range(SEQ_GROUP)]
            first = pl.ds(pl.multiple_of(j * SEQ_GROUP, SEQ_GROUP), SEQ_GROUP)
            for dst, per_seq in ((acc_ref, vals),
                                 (m_ref, [jnp.broadcast_to(o[0], (pad_heads, hd)) for o in outs]),
                                 (l_ref, [jnp.broadcast_to(o[1] * (1.0 / hd), (pad_heads, hd)) for o in outs])):
                for t in range(0, pad_heads, 8):
                    block = jnp.swapaxes(jnp.stack([a[t:t + 8] for a in per_seq], axis=0), 0, 1)
                    for hh in range(t, min(t + 8, heads)):
                        dst[hh, first, :] = block[hh - t]

        def grp_rows(g):
            return pl.ds(pl.multiple_of(g * rows, rows), rows)

        def where_is(idx):
            return (idx // side + core) % CORES, idx % side

        def scores(l, h, idx, buf):
            c, y = where_is(idx)
            for x in range(side):
                s_ref[buf, :, x * shard:(x + 1) * shard] = lax.dot_general(
                    qh[h], kg[l, h, c, y, x], NT, preferred_element_type=F32)

        def soften(h, buf):
            def one(g, carry):
                rs = grp_rows(g)
                hh = h * grp + g
                m_old = m_ref[hh]
                top = [s_ref[buf, rs, j * 128:(j + 1) * 128] for j in range(group_keys // 128)]
                while len(top) > 1:
                    top = [jnp.maximum(a, b) for a, b in zip(top[::2], top[1::2])]
                m_new = jnp.maximum(m_old, jnp.max(top[0], axis=-1, keepdims=True))
                alpha = jnp.exp2((m_old - m_new) * scale2)
                mc = m_new * scale2
                tot = None
                for j in range(group_keys // 128):
                    e = jnp.exp2(s_ref[buf, rs, j * 128:(j + 1) * 128] * scale2 - mc)
                    tot = e if tot is None else tot + e
                    p_ref[buf, rs, j * 128:(j + 1) * 128] = e.astype(BF16)
                m_ref[hh] = m_new
                l_ref[hh] = l_ref[hh] * alpha + tot
                al_ref[buf, rs, :] = alpha
                return carry
            lax.fori_loop(0, grp, one, 0, unroll=True)

        def mix(l, h, idx, buf):
            c, y = where_is(idx)
            pv = None
            for x in range(side):
                d = jnp.dot(p_ref[buf, :, x * shard:(x + 1) * shard], vg[l, h, c, x, y],
                            preferred_element_type=F32)
                pv = d if pv is None else pv + d
            for g in range(grp):
                rs = slice(g * rows, (g + 1) * rows)
                acc_ref[h * grp + g] = acc_ref[h * grp + g] * al_ref[buf, rs, :] + pv[rs]

        def attn_final(h):
            def one(g, carry):
                tot = jnp.sum(l_ref[h * grp + g], axis=-1, keepdims=True)
                hh = h * grp + g
                attn[:, pl.ds(pl.multiple_of(hh * hd, hd), hd)] = (acc_ref[h * grp + g] / tot).astype(BF16)
                return carry
            lax.fori_loop(0, grp, one, 0, unroll=True)

        groups = CORES * side

        def layer(l, carry):
            base = l * per_layer

            def qkv(n, carry):
                r = wtile(base + n, x_out)

                @pl.when(n < qtiles)
                def _():
                    for j in range(heads_per_tile):
                        hh = n * heads_per_tile + j
                        part = r[:, j * hd:(j + 1) * hd]
                        qh[hh // grp, grp_rows(hh % grp), :] = part
                        qs[pl.ds(hh, rows, stride=pad_heads), :] = part.astype(F32)

                def new_rows(new):
                    for h in range(kvh):
                        part = r[:, h * hd:(h + 1) * hd].astype(F32)
                        for d in range(dup):
                            new[l, :, d * kvh + h, :] = part

                @pl.when(n == qtiles)
                def _():
                    new_rows(kn_out)

                @pl.when(n == qtiles + 1)
                def _():
                    new_rows(vn_out)

                @pl.when((l == 0) & (n >= 2) & (n < 2 + kvh))
                def _():
                    x2(n - 2)

                @pl.when((l == 0) & (n >= 2) & (n < kvh))
                def _():
                    x1(n)

                @pl.when((l == 0) & (n == kvh))
                def _():
                    y1(0)

                @pl.when((l == 0) & (n == qtiles + 1))
                def _():
                    y2(0)
                    y1(1)

                @pl.when((l == 1) & (n == 2))
                def _():
                    dd(4)

                @pl.when((l == 1) & (n == qtiles - 1))
                def _():
                    y1(7)

                @pl.when((l == 1) & (n == qtiles + 1))
                def _():
                    dd(5)
                    y2(6)

                return carry
            lax.fori_loop(0, qtiles + 2, qkv, 0)

            def suf(j, carry):
                t = l * ngroups + j
                for cp in scopy(t):
                    cp.wait()
                suffix_group(l, j, t % SUF_SLOTS)

                @pl.when(t + SUF_SLOTS < layers * ngroups)
                def _():
                    for cp in scopy(t + SUF_SLOTS):
                        cp.start()

                @pl.when((l == 0) & (j == ngroups - 1))
                def _():
                    y1(2)

                return carry
            lax.fori_loop(0, ngroups, suf, 0)

            def head(h, carry):
                i = l * kvh + h

                @pl.when(l == 0)
                def _():
                    dd(h)

                @pl.when(i == 6)
                def _():
                    dd(7)

                scores(l, h, 0, 0)
                scores(l, h, 1, 1)
                soften(h, 0)

                def pair(k, carry):
                    @pl.when(k == groups // 4 - 1)
                    def _():
                        ready(i)

                        @pl.when(i == 0)
                        def _():
                            y2(1)
                            y1(3)
                            x1(4)

                        @pl.when(i == 1)
                        def _():
                            y2(2)
                            x2(4)
                            x1(5)

                        @pl.when(i == 2)
                        def _():
                            y2(3)
                            y1(4)
                            x2(5)

                        @pl.when(i == 3)
                        def _():
                            y1(5)
                            x1(6)
                            x1(7)

                        @pl.when(i == 4)
                        def _():
                            dd(6)
                            y2(7)
                    scores(l, h, 2 * k + 2, 0)
                    soften(h, 1)
                    mix(l, h, 2 * k, 0)
                    scores(l, h, 2 * k + 3, 1)
                    soften(h, 0)
                    mix(l, h, 2 * k + 1, 1)
                    return carry
                lax.fori_loop(0, groups // 2 - 1, pair, 0)
                soften(h, 1)
                mix(l, h, groups - 2, 0)
                mix(l, h, groups - 1, 1)

                attn_final(h)

                @pl.when(i == kvh - 1)
                def _():
                    y2(4)
                    x2(6)
                    x2(7)

                return carry
            lax.fori_loop(0, kvh, head, 0)

            def out(n, carry):
                r = wtile(base + qtiles + 2 + n, attn)
                cs = pl.ds(pl.multiple_of(n * TILE_N, TILE_N), TILE_N)
                x_out[:, cs] = (x_out[:, cs].astype(F32) + r.astype(F32)).astype(BF16)

                @pl.when((l == 0) & (n == otiles - 1))
                def _():
                    y2(5)
                    y1(6)

                return carry
            lax.fori_loop(0, otiles, out, 0)
            return carry
        lax.fori_loop(0, layers, layer, 0)

        def drain(i, carry):
            for step in ('x1', 'x2', 'y1', 'y2', 'd'):
                for kind in range(2):
                    for cp in copies(step, kind, i, 1):
                        cp.wait_send()
            return carry
        lax.fori_loop(0, chunks, drain, 0)

    scratch = [
        pltpu.VMEM((layers, kvh, CORES, side, side, shard, hd), BF16),
        pltpu.VMEM((layers, kvh, CORES, side, side, shard, hd), BF16),
        pltpu.VMEM((ring, max(model, qw), TILE_N), BF16),
        pltpu.VMEM((SUF_SLOTS, 2, SEQ_GROUP * srows, hd), BF16),
        pltpu.VMEM((kvh, hrows, hd), BF16),
        pltpu.VMEM((rows * pad_heads, hd), F32),
        pltpu.VMEM((2, hrows, group_keys), F32),
        pltpu.VMEM((2, hrows, group_keys), BF16),
        pltpu.VMEM((heads, rows, hd), F32),
        pltpu.VMEM((heads, rows, hd), F32),
        pltpu.VMEM((heads, rows, hd), F32),
        pltpu.VMEM((2, hrows, hd), F32),
        pltpu.VMEM((rows, qw), BF16),
        pltpu.VMEM((pad_heads, srows), jnp.int32),
        pltpu.VMEM((srows, hd), jnp.int32),
        pltpu.SemaphoreType.DMA((ring,)),
        pltpu.SemaphoreType.DMA((SUF_SLOTS,)),
        pltpu.SemaphoreType.DMA((SUF_SLOTS,)),
        pltpu.SemaphoreType.DMA((2, chunks)),
        pltpu.SemaphoreType.DMA((9, 2, chunks)),
        pltpu.SemaphoreType.DMA((9, 2, chunks)),
    ]
    return kernel, scratch


def fresh_caches(lens_ref, k_ref, v_ref, kn_ref, vn_ref, k_out, v_out, kbuf, vbuf, kn_buf, vn_buf, in_sem, out_sem, new_sem, *, kvh):
    layers, rows = kn_ref.shape[:2]
    slots = k_ref.shape[1] // rows
    n = EPI_GROUP * slots
    steps = rows // EPI_GROUP

    def copies(t, out):
        l, j = t // steps, t % steps
        rs = pl.ds(j * n, n)
        sem = out_sem if out else in_sem
        res = []
        for i, (src, buf, dst) in enumerate(((k_ref, kbuf, k_out), (v_ref, vbuf, v_out))):
            if out:
                res.append(pltpu.make_async_copy(buf.at[t], dst.at[l, rs], sem.at[i, t]))
            else:
                res.append(pltpu.make_async_copy(src.at[l, rs], buf.at[t], sem.at[i, t]))
        return res

    def start(t, carry):
        for cp in copies(t, False):
            cp.start()
        return carry

    def patch(t, carry):
        for cp in copies(t, False):
            cp.wait()
        l, j = t // steps, t % steps
        for b in range(EPI_GROUP):
            sb = j * EPI_GROUP + b
            at = b * slots + lens_ref[sb]
            kbuf[t, at] = kn_buf[l, sb, :kvh, :].astype(BF16)
            vbuf[t, at] = vn_buf[l, sb, :kvh, :].astype(BF16)
        for cp in copies(t, True):
            cp.start()
        return carry

    def finish(t, carry):
        for cp in copies(t, True):
            cp.wait()
        return carry
    news = [pltpu.make_async_copy(kn_ref, kn_buf, new_sem.at[0]), pltpu.make_async_copy(vn_ref, vn_buf, new_sem.at[1])]
    for cp in news:
        cp.start()
    lax.fori_loop(0, layers * steps, start, 0)
    for cp in news:
        cp.wait()
    lax.fori_loop(0, layers * steps, patch, 0)
    lax.fori_loop(0, layers * steps, finish, 0)


def solution(mesh):
    ctx_size = mesh.shape['ctx']
    side = math.isqrt(ctx_size // CORES)
    home_axes = ('data', 'ctx')
    row_spec = P(home_axes, None)
    lens_spec = P(home_axes)
    whole_spec = P()
    prefix_spec = P(None, home_axes, None, None)
    cache_spec = P(None, home_axes, None, None, None)

    def local_step(hidden, seq_lens, w_query, w_key, w_value, w_out, k_prefix, v_prefix, k_suffix, v_suffix):
        layers, shard, kvh, hd = k_prefix.shape
        rows, model = hidden.shape
        slots = k_suffix.shape[2]
        grp = w_query.shape[2] // hd // kvh
        kernel, scratch = build_kernel(layers, kvh, grp, hd, rows, model, shard, slots, side, RING)
        kp = jnp.swapaxes(k_prefix, 1, 2)
        vp = jnp.swapaxes(v_prefix, 1, 2)
        ks = k_suffix.reshape(layers, rows * slots * kvh, hd)
        vs = v_suffix.reshape(layers, rows * slots * kvh, hd)
        vmem = pl.BlockSpec(memory_space=pltpu.VMEM)
        hbm = pl.BlockSpec(memory_space=pl.ANY)
        x_new, k_new, v_new = pl.pallas_call(
            kernel,
            out_shape=(jax.ShapeDtypeStruct((rows, model), BF16),
                       jax.ShapeDtypeStruct((layers, rows, 8, hd), F32),
                       jax.ShapeDtypeStruct((layers, rows, 8, hd), F32)),
            in_specs=[pl.BlockSpec(memory_space=pltpu.SMEM), vmem] + [hbm] * 8,
            out_specs=(vmem, vmem, vmem),
            scratch_shapes=scratch,
            compiler_params=pltpu.CompilerParams(
                collective_id=0, has_side_effects=True, vmem_limit_bytes=67043328),
        )(seq_lens, hidden, w_query, w_key, w_value, w_out, kp, vp, ks, vs)
        steps = layers * (rows // EPI_GROUP)
        flat = (layers, rows * slots, kvh, hd)
        k_out, v_out = pl.pallas_call(
            functools.partial(fresh_caches, kvh=kvh),
            out_shape=(jax.ShapeDtypeStruct(flat, BF16),) * 2,
            in_specs=[pl.BlockSpec(memory_space=pltpu.SMEM), hbm, hbm]
            + [pl.BlockSpec(memory_space=pltpu.HBM)] * 2,
            out_specs=(hbm, hbm),
            scratch_shapes=[pltpu.VMEM((steps, EPI_GROUP * slots, kvh, hd), BF16)] * 2
            + [pltpu.VMEM(k_new.shape, F32)] * 2 + [pltpu.SemaphoreType.DMA((2, steps))] * 2
            + [pltpu.SemaphoreType.DMA((2,))],
            compiler_params=pltpu.CompilerParams(vmem_limit_bytes=48 * 2 ** 20),
        )(seq_lens, k_suffix.reshape(flat), v_suffix.reshape(flat), k_new, v_new)
        k_out = k_out.reshape(k_suffix.shape)
        v_out = v_out.reshape(v_suffix.shape)
        return x_new, k_out, v_out

    return jax.shard_map(
        local_step, mesh=mesh,
        in_specs=(row_spec, lens_spec, whole_spec, whole_spec, whole_spec, whole_spec,
                  prefix_spec, prefix_spec, cache_spec, cache_spec),
        out_specs=(row_spec, cache_spec, cache_spec), check_vma=False)
```
